256 devices in a mesh: grp: 2 (over z), kvp: 16 (over x, core), tp: 8 (over y).
Axes of the slice: x: 8, y: 8, z: 2, core: 2. Of those that a mesh axis runs over, the one named last changes fastest.
The devices are a block of a 8x8x16 slice.
Arguments:
- hidden_in: bfloat16 [16, 7168], P('grp'), parts along dimension 0, may hold values from -3 to 3
- queries_nope: bfloat16 [16, 128, 128], P('grp', ('kvp', 'tp')), parts along dimension 0, may hold values from -6 to 6
- queries_rope: bfloat16 [16, 128, 64], P('grp', ('kvp', 'tp')), parts along dimension 0, may hold values from -26 to 26
- cache: bfloat16 [16, 6144, 576], P('grp', 'kvp'), parts along dimension 0, may hold values from -20 to 20
- lengths: int32 [16], P('grp'), parts along dimension 0, may hold values from 128 to 6144, as said below
- w_uk: bfloat16 [128, 128, 512], P(('kvp', 'tp')), may hold values from -0.5 to 0.5
- w_uv: bfloat16 [128, 512, 128], P(('kvp', 'tp')), may hold values from -0.25 to 0.25
- w_out: bfloat16 [16384, 7168], P(('kvp', 'tp')), may hold values from -0.1875 to 0.1875
- norm_gain: float32 [7168], replicated, may hold values from 0.25 to 1.75
- w_gate: bfloat16 [7168, 18432], P(None, ('kvp', 'tp')), may hold values from -0.0625 to 0.0625
- w_up: bfloat16 [7168, 18432], P(None, ('kvp', 'tp')), may hold values from -0.0625 to 0.0625
- w_down: bfloat16 [18432, 7168], P(('kvp', 'tp')), may hold values from -0.15625 to 0.15625
Outputs:
- layer_out: bfloat16 [16, 7168], P('grp', ('kvp', 'tp')), parts along dimension 0
The draws below stay inside these ranges and needn't reach their ends.
There are 2 independent parts, one for each index of `grp`. The reference program is written for one: setup_inputs(seed, part) draws one part's arguments, and reference() takes and returns one part's arrays. A program takes and returns all parts, laid end to end along the dimension named above; an argument that names none is the same for every part. Nothing has to cross between parts.
Inputs may be any that keep to these rules, and one draw needn't show every extreme that they name: `lengths`: every length is a multiple of 128; in every draw some request has the full 6144.
All inputs are finite; a program needn't handle non-finite values.
Results may differ from the reference program's by a relative error of at most 0.04.
Values may be sent and summed in bfloat16 or wider, within the bound.
A program may use at most 64 MiB of HBM per device.

```python
import jax
import jax.numpy as jnp
from jax import lax

D = 7168
FF = 18432
H = 128
LAT = 512
ROPE = 64
HEAD_DIM = 128
BATCH = 8
BLOCK = 128
CTX_DEV = 384
CTX = 6144
N_KVP = 16


def draw_lengths(key, part):
    count_blocks = CTX // BLOCK
    counts = jax.random.randint(key, (BATCH,), 1, count_blocks + 1)
    full_row = jax.random.randint(jax.random.fold_in(key, 3), (), 0, BATCH)
    counts = jnp.where(jnp.arange(BATCH) == full_row, count_blocks, counts)
    return (counts * BLOCK).astype(jnp.int32)


def draw_cache(key, part):
    values = jnp.clip(jax.random.normal(jax.random.fold_in(key, 11), (BATCH, CTX, LAT + ROPE), jnp.float32), -6.0, 6.0)
    return values.astype(jnp.bfloat16)


def draw_queries_rope(key, part):
    values = jnp.clip(jax.random.normal(jax.random.fold_in(key, 21), (BATCH, H, ROPE), jnp.float32), -6.0, 6.0)
    return values.astype(jnp.bfloat16)


def strengthened(drawn, key, source, target, shards_of, factor):
    def block_of(position):
        return (jnp.arange(drawn.shape[position]) // (drawn.shape[position] // shards_of)).reshape((-1,) + (1,) * (drawn.ndim - 1 - position))

    first = jax.random.permutation(key, shards_of)[block_of(target)]
    far = (block_of(target) + shards_of // 2) % shards_of
    return jnp.where((block_of(source) == first) | (block_of(source) == far), factor * drawn, drawn)


def block_scale(own_key, shape, pieces, smallest, largest):
    level = 1.0
    for position, shards_of in pieces:
        heights = jax.random.uniform(jax.random.fold_in(jax.random.fold_in(own_key, 6), position), (shards_of,), jnp.float32, smallest / len(pieces), largest / len(pieces))
        level = level * jnp.repeat(jnp.exp(heights), shape[position] // shards_of).reshape((-1,) + (1,) * (len(shape) - 1 - position))
    return level


def centred(own_key, extent, scale, most, shards=(), kind=jnp.bfloat16):
    result = jax.random.normal(own_key, extent, jnp.float32) * scale
    if len(shards) > 0:
        result = block_scale(own_key, extent, shards, -0.22, 0.18) * result
    return jnp.clip(result, min=-most, max=most).astype(kind)


def heavy_noise(own_key, extent, deviation, bound, cuts, heavy, kind=jnp.bfloat16):
    entries = deviation * jax.random.normal(own_key, extent, jnp.float32)
    if cuts:
        entries = entries * block_scale(own_key, extent, cuts, -0.22, 0.18)
    return jnp.clip(strengthened(entries, jax.random.fold_in(own_key, 3), *heavy), -bound, bound).astype(kind)


def setup_inputs(seed: int = 0, part: int = 0) -> dict:
    key_of = jax.random.split(jax.random.key(seed), 13)
    own_keys = jax.random.split(jax.random.fold_in(key_of[12], part), 13)
    hidden_in = centred(own_keys[0], (BATCH, D), 0.5, 3.0)
    queries_nope = centred(own_keys[1], (BATCH, H, HEAD_DIM), 1.0, 6.0, ((1, 128),))
    queries_rope = draw_queries_rope(jax.random.fold_in(jax.random.fold_in(key_of[12], part), 71), part)
    cache = draw_cache(jax.random.fold_in(jax.random.fold_in(key_of[12], part), 71), part)
    lengths = draw_lengths(jax.random.fold_in(jax.random.fold_in(key_of[12], part), 71), part)
    w_uk = centred(key_of[5], (H, HEAD_DIM, LAT), HEAD_DIM ** -0.5, 0.5, ((0, 128),))
    w_uv = centred(key_of[6], (H, LAT, HEAD_DIM), LAT ** -0.5, 0.25, ((0, 128),))
    w_out = heavy_noise(key_of[7], (H * HEAD_DIM, D), (H * HEAD_DIM) ** -0.5, 0.1875, ((0, 128),), (0, 1, 128, 5.5))
    norm_gain = jnp.clip(1.0 + 0.15 * jax.random.normal(key_of[8], (D,), jnp.float32), 0.25, 1.75)
    w_gate = centred(key_of[9], (D, FF), D ** -0.5, 0.0625, ((1, 128),))
    w_up = centred(key_of[10], (D, FF), D ** -0.5, 0.0625, ((1, 128),))
    w_down = heavy_noise(key_of[11], (FF, D), FF ** -0.5, 0.15625, ((0, 128),), (0, 1, 128, 5.5))
    return {"hidden_in": hidden_in, "queries_nope": queries_nope, "queries_rope": queries_rope, "cache": cache, "lengths": lengths, "w_uk": w_uk, "w_uv": w_uv, "w_out": w_out, "norm_gain": norm_gain, "w_gate": w_gate, "w_up": w_up, "w_down": w_down}


def reference(hidden_in, queries_nope, queries_rope, cache, lengths, w_uk, w_uv, w_out, norm_gain, w_gate, w_up, w_down):
    score_scale = float(HEAD_DIM + ROPE) ** (-0.5)
    q_lat = jnp.einsum('bhd,hdl->bhl', queries_nope.astype(jnp.float32), w_uk.astype(jnp.float32)).astype(jnp.bfloat16)
    q_full = jnp.concatenate([q_lat, queries_rope], axis=2).astype(jnp.float32)
    cache_wide = cache.astype(jnp.float32)
    scores = jnp.einsum('bhc,btc->bht', q_full, cache_wide) * score_scale
    visible = jnp.arange(CTX, dtype=jnp.int32)[None, :] < lengths[:, None]
    visible = jnp.broadcast_to(visible[:, None, :], scores.shape).reshape(BATCH, H, N_KVP, CTX_DEV)
    blocks = scores.reshape(BATCH, H, N_KVP, CTX_DEV)
    masked = jnp.where(visible, blocks, jnp.float32(-1e+30))
    block_max = lax.optimization_barrier(jnp.max(masked, axis=3))
    exponent = jnp.where(visible, jnp.exp(masked - block_max[..., None]), jnp.float32(0.0))
    block_sum = lax.optimization_barrier(jnp.sum(exponent, axis=3))
    guarded = jnp.maximum(block_sum, 1.0)
    log_total = block_max + jnp.log(guarded)
    weights = (exponent / guarded[..., None]).astype(jnp.bfloat16)
    cache_blocks = cache_wide.reshape(BATCH, N_KVP, CTX_DEV, LAT + ROPE)
    partial_value = jnp.einsum('bhkt,bktc->bhkc', weights.astype(jnp.float32), cache_blocks)[..., :LAT]
    highest = lax.optimization_barrier(jnp.max(log_total, axis=2))
    overall = highest + jnp.log(lax.optimization_barrier(jnp.sum(jnp.exp(log_total - highest[..., None]), axis=2)))
    o_lat = lax.optimization_barrier(jnp.sum(jnp.exp(log_total - overall[..., None])[..., None] * partial_value, axis=2)).astype(jnp.bfloat16)
    head_out = jnp.einsum('bhl,hle->bhe', o_lat.astype(jnp.float32), w_uv.astype(jnp.float32)).astype(jnp.bfloat16)
    attention = jnp.dot(head_out.reshape(BATCH, H * HEAD_DIM), w_out, preferred_element_type=jnp.float32)
    residual = hidden_in.astype(jnp.float32) + attention
    mean_square = lax.optimization_barrier(jnp.mean(residual * residual, axis=1))
    normed = (residual * lax.rsqrt(mean_square + 1e-06)[:, None] * norm_gain.astype(jnp.float32)[None, :]).astype(jnp.bfloat16)
    gate_proj = jnp.dot(normed, w_gate, preferred_element_type=jnp.float32)
    up_proj = jnp.dot(normed, w_up, preferred_element_type=jnp.float32)
    act = (jax.nn.silu(gate_proj) * up_proj).astype(jnp.bfloat16)
    ffn_out = jnp.dot(act, w_down, preferred_element_type=jnp.float32)
    return (residual + ffn_out).astype(jnp.bfloat16)
```

```python
import functools

import jax
import jax.numpy as jnp
from jax import lax
from jax.experimental import pallas as pl
from jax.experimental.pallas import tpu as pltpu
from jax.sharding import PartitionSpec as P

MESH = pl.DeviceIdType.MESH
BF16 = jnp.bfloat16
F32 = jnp.float32
LANES = 128
CORES = 2


def rows_of(core, first, second):
    return jnp.where(core == 0, first, second)


def kernel(
    n_kvp,
    n_tp,
    hidden_hbm,
    qn_hbm,
    qr_hbm,
    cache_hbm,
    lengths_hbm,
    wuk_hbm,
    wuv_hbm,
    wout_hbm,
    gain_hbm,
    wg_hbm,
    wu_hbm,
    wd_hbm,
    out_ref,
    hidden,
    qn,
    qr,
    cache,
    lengths,
    wuk,
    wuv,
    wout,
    gain,
    wg,
    wu,
    wd,
    qbuf,
    psend,
    pbuf,
    d1_mine,
    d1_send,
    d1_recv,
    rs1_send,
    rs1_recv,
    ag_own,
    ag_other,
    res,
    d2_mine,
    d2_send,
    d2_recv,
    rs2_send,
    rs2_recv,
    sw_send,
    sw_recv,
    load_sem,
    send_sem,
    recv_sem,
    sync_sem,
):
    k = lax.axis_index("kvp")
    t = lax.axis_index("tp")
    x, c = k // CORES, k % CORES
    n_x = n_kvp // CORES
    n_chips = n_x * n_tp
    batch, width = hidden.shape
    half = batch // 2
    latent = wuk.shape[1]
    rope = qr.shape[1]
    ctx_dev = cache.shape[2]
    n_tiles = width // LANES
    share = width // (n_kvp * n_tp)
    chip = x * n_tp + t
    per_row = n_tiles // n_x

    def device(px, pc, py):
        return {"kvp": px * CORES + pc, "tp": py}

    def load(i, src, dst):
        copy = pltpu.make_async_copy(src, dst, load_sem.at[i])
        copy.start()
        return copy

    l_qn = load(0, qn_hbm, qn)
    l_wuk = load(1, wuk_hbm, wuk)
    l_qr = load(2, qr_hbm, qr)
    l_len = load(3, lengths_hbm, lengths)
    l_cache = load(4, cache_hbm, cache)
    l_wuv = load(5, wuv_hbm, wuv)
    l_wout = load(6, wout_hbm, wout)
    l_hidden = load(7, hidden_hbm, hidden)
    l_gain = load(8, gain_hbm, gain)
    l_wg = load(9, wg_hbm, wg)
    l_wu = load(10, wu_hbm, wu)
    l_wd = load(11, wd_hbm, wd)

    barrier = pltpu.get_barrier_semaphore()
    for i in range(1, n_kvp):
        pl.semaphore_signal(
            barrier, inc=1, device_id={"kvp": (k + i) % n_kvp, "tp": t}, device_id_type=MESH
        )
    for i in range(1, n_tp):
        pl.semaphore_signal(
            barrier, inc=1, device_id={"kvp": k, "tp": (t + i) % n_tp}, device_id_type=MESH
        )

    l_qn.wait()
    l_wuk.wait()
    l_qr.wait()
    q_lat = jnp.dot(qn[...], wuk[...], preferred_element_type=F32).astype(BF16)
    qbuf[k, :, :latent] = q_lat
    qbuf[k, :, latent:] = jnp.concatenate(
        [qr[...], jnp.zeros((batch, qbuf.shape[2] - latent - rope), BF16)], axis=1
    )
    pl.semaphore_wait(barrier, n_kvp - 1 + n_tp - 1)

    order = sorted(range(1, n_kvp), key=lambda i: abs(i - n_kvp // 2))

    def to_kvp(src, dst, phase):
        for i in order:
            peer = (k + i) % n_kvp
            pltpu.make_async_remote_copy(
                src(peer),
                dst,
                send_sem.at[phase],
                recv_sem.at[phase],
                device_id={"kvp": peer, "tp": t},
                device_id_type=MESH,
            ).start()

    def bulk(ref, phase):
        return pltpu.make_async_remote_copy(
            ref,
            ref,
            send_sem.at[phase],
            recv_sem.at[phase],
            device_id=device(x, 1 - c, t),
            device_id_type=MESH,
        )

    to_kvp(lambda peer: qbuf.at[k], qbuf.at[k], 0)
    for i in range(1, n_tp):
        pl.semaphore_signal(
            sync_sem, inc=1, device_id={"kvp": k, "tp": (t + i) % n_tp}, device_id_type=MESH
        )

    l_len.wait()
    row = lax.broadcasted_iota(jnp.int32, (batch, ctx_dev), 0)
    position = lax.broadcasted_iota(jnp.int32, (batch, ctx_dev), 1) + k * ctx_dev
    length = jnp.zeros((batch, ctx_dev), jnp.int32)
    for b in range(batch):
        length = jnp.where(row == b, lengths[b], length)
    visible = (position < length)[None]
    row = row[None]
    l_cache.wait()
    bulk(qbuf.at[pl.ds(0, n_kvp - 1)], 0).wait_recv()

    rows = n_kvp * batch
    queries = qbuf[...].astype(F32).reshape(rows, qbuf.shape[2]).astype(BF16)
    queries = queries[:, : latent + rope]
    scale = float(qn.shape[1] + rope) ** (-0.5)
    scores = jnp.zeros((n_kvp, batch, ctx_dev), F32)
    for b in range(batch):
        s_b = jnp.dot(queries, cache[b], preferred_element_type=F32)
        scores = jnp.where(row == b, s_b.reshape(n_kvp, batch, ctx_dev), scores)
    masked = jnp.where(visible, scores * scale, F32(-1e30))
    block_max = jnp.max(masked, axis=2, keepdims=True)
    exps = jnp.where(visible, jnp.exp(masked - block_max), F32(0.0))
    guarded = jnp.maximum(jnp.sum(exps, axis=2, keepdims=True), 1.0)
    log_total = block_max + jnp.log(guarded)
    weights = exps / guarded
    partial = jnp.zeros((rows, latent), F32)
    for b in range(batch):
        w_b = jnp.where(row == b, weights, F32(0.0)).reshape(rows, ctx_dev).astype(BF16)
        partial += lax.dot_general(
            w_b, cache[b, :latent, :], (((1,), (1,)), ((), ())), preferred_element_type=F32
        )
    log_high = log_total.astype(BF16).astype(F32)
    log_low = log_total - log_high
    lane = lax.broadcasted_iota(jnp.int32, (n_kvp, batch, LANES), 2)
    logs = jnp.where(lane == 0, log_high, jnp.where(lane == 1, log_low, F32(0.0)))
    psend[:, :, :latent] = partial.reshape(n_kvp, batch, latent).astype(BF16)
    psend[:, :, latent:] = logs.astype(BF16)
    pbuf[k] = psend[k]
    to_kvp(lambda peer: psend.at[peer], pbuf.at[k], 1)
    l_wuv.wait()
    l_wout.wait()
    bulk(pbuf.at[pl.ds(0, n_kvp - 1)], 1).wait_recv()

    parts = pbuf[...].astype(F32)
    part_logs = parts[:, :, latent : latent + 1] + parts[:, :, latent + 1 : latent + 2]
    shifted = jnp.exp(part_logs - jnp.max(part_logs, axis=0, keepdims=True))
    coef = shifted / jnp.sum(shifted, axis=0, keepdims=True)
    o_lat = jnp.sum(coef * parts[:, :, :latent], axis=0).astype(BF16)
    head_out = jnp.dot(o_lat, wuv[...], preferred_element_type=F32).astype(BF16)
    attention = jnp.dot(head_out, wout[...], preferred_element_type=F32)

    for j in range(n_tiles):
        tile = attention[:, j * LANES : (j + 1) * LANES]
        d1_mine[j] = rows_of(c, tile[:half], tile[half:])
        d1_send[j] = rows_of(c, tile[half:], tile[:half]).astype(BF16)

    def swap(src, dst, phase):
        copy = pltpu.make_async_remote_copy(
            src,
            dst,
            send_sem.at[phase],
            recv_sem.at[phase],
            device_id=device(x, 1 - c, t),
            device_id_type=MESH,
        )
        copy.start()
        return copy

    s1 = swap(d1_send, d1_recv, 2)
    s1.wait_recv()
    rs1_send[...] = (d1_mine[...] + d1_recv[...].astype(F32)).astype(BF16)
    pl.semaphore_wait(sync_sem, n_tp - 1)

    def to_chips(start_one):
        def step(i, _):
            px = (x + n_x // 2 + i // n_tp) % n_x
            py = (t + n_tp // 2 + i % n_tp) % n_tp
            start_one(px, py)
            return 0

        middle = (n_x // 2) * n_tp + n_tp // 2
        lax.fori_loop(0, middle, step, 0)
        lax.fori_loop(middle + 1, n_chips, step, 0)

    def slot_of(px, py):
        return (px + py) % n_x, px * per_row + (px + py) % n_x

    my_place, my_tile = slot_of(x, t)
    owner = my_place < per_row

    def rs1_one(px, py):
        place, tile = slot_of(px, py)

        @pl.when(place < per_row)
        def _():
            pltpu.make_async_remote_copy(
                rs1_send.at[tile],
                rs1_recv.at[chip],
                send_sem.at[3],
                recv_sem.at[3],
                device_id=device(px, c, py),
                device_id_type=MESH,
            ).start()

    to_chips(rs1_one)
    l_hidden.wait()

    def ag_one(px, py):
        pltpu.make_async_remote_copy(
            ag_own.at[my_tile],
            ag_own.at[my_tile],
            send_sem.at[4],
            recv_sem.at[4],
            device_id=device(px, c, py),
            device_id_type=MESH,
        ).start()

    @pl.when(owner)
    def _():
        rs1_recv[chip] = rs1_send[my_tile]
        mine = hidden[:, pl.ds(pl.multiple_of(my_tile * LANES, LANES), LANES)].astype(F32)
        mine = rows_of(c, mine[:half], mine[half:])
        bulk(rs1_recv.at[pl.ds(0, n_chips - 1)], 3).wait_recv()
        total = mine + jnp.sum(rs1_recv[...].astype(F32), axis=0)
        ag_own[my_tile] = total.astype(BF16)
        to_chips(ag_one)
        bulk(ag_own.at[pl.ds(0, n_tiles - 1)], 4).wait_recv()

    @pl.when(jnp.logical_not(owner))
    def _():
        bulk(ag_own.at[pl.ds(0, n_tiles)], 4).wait_recv()

    s2 = swap(ag_own, ag_other, 5)
    l_gain.wait()
    l_wg.wait()
    l_wu.wait()
    s2.wait_recv()

    own = ag_own[...].astype(F32)
    other = ag_other[...].astype(F32)
    residual = jnp.concatenate([rows_of(c, own, other), rows_of(c, other, own)], axis=1)
    res[:n_tiles] = residual
    res[n_tiles] = jnp.zeros((batch, LANES), F32)
    squares = jnp.sum(jnp.sum(residual * residual, axis=0), axis=1, keepdims=True)
    inverse = lax.rsqrt(squares / width + 1e-6)
    normed = residual * inverse[None] * gain[...][:, None, :]
    normed = jnp.concatenate([normed[j] for j in range(n_tiles)], axis=1).astype(BF16)
    dims = (((1,), (1,)), ((), ()))
    gate_proj = lax.dot_general(wg[...], normed, dims, preferred_element_type=F32)
    up_proj = lax.dot_general(wu[...], normed, dims, preferred_element_type=F32)
    act = gate_proj / (1.0 + jnp.exp(-gate_proj)) * up_proj
    act = act.T.astype(BF16)
    l_wd.wait()
    ffn = jnp.dot(act, wd[...], preferred_element_type=F32)

    pad = jnp.zeros((batch, LANES - CORES * share), F32)
    for px in range(n_x):
        for py in range(n_tp):
            first = share * (CORES * px * n_tp + py)
            second = first + share * n_tp
            tile = jnp.concatenate(
                [ffn[:, first : first + share], ffn[:, second : second + share], pad], axis=1
            )
            slot = px * n_tp + py
            d2_mine[slot] = rows_of(c, tile[:half], tile[half:])
            d2_send[slot] = rows_of(c, tile[half:], tile[:half]).astype(BF16)
    s3 = swap(d2_send, d2_recv, 6)
    s3.wait_recv()
    rs2_send[...] = (d2_mine[...] + d2_recv[...].astype(F32)).astype(BF16)

    def rs2_one(px, py):
        pltpu.make_async_remote_copy(
            rs2_send.at[px * n_tp + py],
            rs2_recv.at[chip],
            send_sem.at[7],
            recv_sem.at[7],
            device_id=device(px, c, py),
            device_id_type=MESH,
        ).start()

    to_chips(rs2_one)
    rs2_recv[chip] = rs2_send[chip]
    start = share * (k * n_tp + t)
    base = start // LANES
    near = jnp.concatenate([res[base], res[base + 1]], axis=1)
    near = pltpu.roll(near, 2 * LANES - start % LANES, 1)[:, :share]
    bulk(rs2_recv.at[pl.ds(0, n_chips - 1)], 7).wait_recv()
    total = jnp.sum(rs2_recv[...].astype(F32), axis=0)
    sw_send[...] = total
    s4 = swap(sw_send, sw_recv, 8)
    s4.wait_recv()
    peer = sw_recv[...]
    whole = jnp.concatenate([rows_of(c, total, peer), rows_of(c, peer, total)], axis=0)
    mine = rows_of(c, whole[:, :share], whole[:, share : 2 * share])
    out_ref[...] = (near + mine).astype(BF16)

    bulk(qbuf.at[pl.ds(0, n_kvp - 1)], 0).wait_send()
    bulk(pbuf.at[pl.ds(0, n_kvp - 1)], 1).wait_send()
    s1.wait_send()

    @pl.when(owner)
    def _():
        bulk(rs1_send.at[pl.ds(0, n_tiles - 1)], 3).wait_send()
        bulk(rs1_recv.at[pl.ds(0, n_chips - 1)], 4).wait_send()

    @pl.when(jnp.logical_not(owner))
    def _():
        bulk(rs1_send, 3).wait_send()

    s2.wait_send()
    s3.wait_send()
    bulk(rs2_send.at[pl.ds(0, n_chips - 1)], 7).wait_send()
    s4.wait_send()


def per_device(n_kvp, n_tp, *args):
    hidden, qn, qr, cache, lengths, wuk, wuv, wout, gain, wg, wu, wd = args
    batch, width = hidden.shape
    half = batch // 2
    n_chips = n_kvp // CORES * n_tp
    n_tiles = width // LANES
    latent = wuk.shape[2]
    lanes = latent + LANES
    operands = (
        hidden,
        qn.reshape(batch, qn.shape[2]),
        qr.reshape(batch, qr.shape[2]),
        cache.transpose(0, 2, 1),
        lengths,
        wuk.reshape(wuk.shape[1:]),
        wuv.reshape(wuv.shape[1:]),
        wout,
        gain.reshape(n_tiles, LANES),
        wg.T,
        wu.T,
        wd,
    )
    spaces = [pltpu.SMEM if a is lengths else pltpu.VMEM for a in operands]
    share = width // (n_kvp * n_tp)
    return pl.pallas_call(
        functools.partial(kernel, n_kvp, n_tp),
        name="layer",
        out_shape=jax.ShapeDtypeStruct((batch, share), BF16),
        in_specs=[pl.BlockSpec(memory_space=pl.ANY)] * len(operands),
        out_specs=pl.BlockSpec(memory_space=pltpu.VMEM),
        scratch_shapes=[
            *(space(a.shape, a.dtype) for space, a in zip(spaces, operands)),
            pltpu.VMEM((n_kvp, batch, lanes), BF16),
            pltpu.VMEM((n_kvp, batch, lanes), BF16),
            pltpu.VMEM((n_kvp, batch, lanes), BF16),
            pltpu.VMEM((n_tiles, half, LANES), F32),
            pltpu.VMEM((n_tiles, half, LANES), BF16),
            pltpu.VMEM((n_tiles, half, LANES), BF16),
            pltpu.VMEM((n_tiles, half, LANES), BF16),
            pltpu.VMEM((n_chips, half, LANES), BF16),
            pltpu.VMEM((n_tiles, half, LANES), BF16),
            pltpu.VMEM((n_tiles, half, LANES), BF16),
            pltpu.VMEM((n_tiles + 1, batch, LANES), F32),
            pltpu.VMEM((n_chips, half, LANES), F32),
            pltpu.VMEM((n_chips, half, LANES), BF16),
            pltpu.VMEM((n_chips, half, LANES), BF16),
            pltpu.VMEM((n_chips, half, LANES), BF16),
            pltpu.VMEM((n_chips, half, LANES), BF16),
            pltpu.VMEM((half, LANES), F32),
            pltpu.VMEM((half, LANES), F32),
            pltpu.SemaphoreType.DMA((len(operands),)),
            pltpu.SemaphoreType.DMA((9,)),
            pltpu.SemaphoreType.DMA((9,)),
            pltpu.SemaphoreType.REGULAR,
        ],
        compiler_params=pltpu.CompilerParams(
            collective_id=0, has_side_effects=True, vmem_limit_bytes=60 * 1024 * 1024
        ),
    )(*operands)


def solution(mesh):
    n_kvp, n_tp = mesh.shape["kvp"], mesh.shape["tp"]
    both = ("kvp", "tp")
    return jax.shard_map(
        functools.partial(per_device, n_kvp, n_tp),
        mesh=mesh,
        in_specs=(
            P("grp", None),
            P("grp", both, None),
            P("grp", both, None),
            P("grp", "kvp", None),
            P("grp"),
            P(both, None, None),
            P(both, None, None),
            P(both, None),
            P(),
            P(None, both),
            P(None, both),
            P(both, None),
        ),
        out_specs=P("grp", both),
        check_vma=False,
    )
```
